32 devices in a mesh: colour: 2 (over core), sub: 16 (over z, y, x).
Axes of the slice: x: 2, y: 2, z: 4, core: 2. Of those that a mesh axis runs over, the one named last changes fastest.
Arguments:
- rhs: float32 [3, 64, 256, 512], P(None, 'sub'), may hold values from -60 to 60
- diagonal: float32 [64, 256, 512], P('sub'), may hold values from 0.2 to 6
Outputs:
- solution: float32 [3, 64, 256, 512], P(None, 'sub', None, 'colour')
- residual: float32 [3, 64, 256, 512], P(None, 'sub', None, 'colour')
- norms: float32 [3], replicated
The draws below stay inside these ranges and needn't reach their ends.
All inputs are finite; a program needn't handle non-finite values.
Results may differ from the reference program's by a relative error of at most 0.0003.
Values sent between devices are 32-bit elements; how exact they have to be, the bound alone decides.
A program may use at most 128 MiB of HBM per device.

```python
import math
import jax
import jax.numpy as jnp
from jax import lax

CX = 4
NY = 256
NZ = 512
RIM = 1
SWEEPS = 8
NRHS = 3
NX = 64
N_SUB = 16


def draw_rhs(key, part):
    first = jax.random.fold_in(jax.random.fold_in(key, 17), 0)
    base = jax.random.normal(first, (NRHS, NX, NY, NZ), jnp.float32)
    ramp = 1.0 + 2.0 * jnp.arange(NX, dtype=jnp.float32) / (NX - 1)
    ramp = ramp[None, :, None, None]
    field = base * ramp
    return jnp.clip(field, -60.0, 60.0)


def level_of(rng, extent, shards, low, largest):
    gain = 1.0
    for axis_at, parts in shards:
        steps = jax.random.uniform(jax.random.fold_in(jax.random.fold_in(rng, 6), axis_at), (parts,), jnp.float32, low / len(shards), largest / len(shards))
        gain = gain * jnp.repeat(jnp.exp(steps), extent[axis_at] // parts).reshape((-1,) + (1,) * (len(extent) - 1 - axis_at))
    return gain


def setup_inputs(seed: int = 0) -> dict:
    seeds = jax.random.split(jax.random.key(seed), 3)
    return {
        "rhs": draw_rhs(jax.random.fold_in(seeds[2], 71), 0),
        "diagonal": jnp.clip(jnp.exp(math.log(6.0) - 3.4011974 * jax.random.uniform(seeds[1], (NX, NY, NZ), jnp.float32) ** level_of(seeds[1], (NX, NY, NZ), ((0, 16),), -0.2, 0.2)), 0.2, 6.0),
    }


OMEGA = 0.8

def neighbours(field):
    pads = ((0, 0),) * (field.ndim - 3) + ((1, 1), (1, 1), (1, 1))
    padded = jnp.pad(field, pads)
    beside = padded[..., 2:, 1:-1, 1:-1] + padded[..., :-2, 1:-1, 1:-1]
    beside = beside + padded[..., 1:-1, 2:, 1:-1] + padded[..., 1:-1, :-2, 1:-1]
    beside = beside + padded[..., 1:-1, 1:-1, 2:] + padded[..., 1:-1, 1:-1, :-2]
    return beside

def jacobi(resid, diag, mask):
    scale = OMEGA / (6.0 + diag)
    found = jnp.zeros_like(resid)
    for sweep in range(SWEEPS):
        found = (found + scale * (resid - (6.0 + diag) * found + neighbours(found))) * mask
    return found

def operate(field, diagonal):
    return (6.0 + diagonal) * field - neighbours(field)

def reference(rhs, diagonal):
    half = CX // 2
    span = half + 2 * RIM
    padded_diag = jnp.pad(diagonal, ((RIM, RIM), (0, 0), (0, 0)))
    layouts = []
    for colour in range(2):
        starts = jnp.arange(N_SUB, dtype=jnp.int32) * CX + colour * half
        index = (starts[:, None] + jnp.arange(span, dtype=jnp.int32)[None, :]).astype(jnp.int32)
        place = index - RIM
        mask = ((place >= 0) & (place < NX)).astype(jnp.float32)[:, :, None, None]
        layouts.append((index, mask, padded_diag[index]))

    def correction(resid, layout):
        index, mask, diag_regions = layout
        padded = jnp.pad(resid, ((RIM, RIM), (0, 0), (0, 0)))
        regions = padded[index] * mask
        found = jacobi(regions, diag_regions, mask)
        total = jnp.zeros_like(padded).at[index.reshape(-1)].add(found.reshape(-1, NY, NZ))
        return total[RIM:RIM + NX]

    def one_rhs(source):
        current = jnp.zeros_like(source)
        resid = source
        for colour in range(2):
            corr = correction(resid, layouts[colour])
            image = operate(corr, diagonal)
            alpha = jnp.sum(resid * corr) / jnp.sum(corr * image)
            current = current + alpha * corr
            resid = resid - alpha * image
        return (current, resid, jnp.sqrt(jnp.sum(resid * resid)))
    solution, residual, norms = lax.map(one_rhs, rhs)
    return (solution, residual, norms)
```

```python
import functools

import jax
import jax.numpy as jnp
from jax import lax
from jax.experimental import pallas as pl
from jax.experimental.pallas import tpu as pltpu
from jax.sharding import PartitionSpec as P

SWEEPS = 8
OMEGA = 0.8
RIM = 2 * SWEEPS
ROWS = 8
LANES = 128


def shift(value, last, axis, step):
    size = value.shape[axis]
    at = lax.broadcasted_iota(jnp.int32, value.shape, axis)
    if step > 0:
        return pltpu.roll(jnp.where(at == size - 1, last, value), 1, axis)
    return pltpu.roll(jnp.where(at == 0, last, value), size - 1, axis)


def lateral(planes, p, t, before, after):
    row = planes[p]
    zero = jnp.zeros_like(row[t])
    low = row[t - 1] if t > 0 else zero
    high = row[t + 1] if t + 1 < len(row) else zero
    total = shift(row[t], before, 0, 1) + shift(row[t], after, 0, -1)
    return total + (shift(row[t], low, 1, 1) + shift(row[t], high, 1, -1))


def lane(t):
    return slice(t * LANES, (t + 1) * LANES)


def solve_kernel(order, extra_ref, resid_ref, scale_ref, lo_ref, hi_ref, sq, ea, eb):
    _, rows, depth = scale_ref.shape
    tiles = depth // LANES
    span = len(order)
    refs = [(extra_ref, 0) if at < 0 else (resid_ref, at) for at in order]
    blank = jnp.zeros((span, ROWS, depth), jnp.float32)
    for buf in (ea, eb):
        buf[:, :ROWS, :] = blank
        buf[:, rows + ROWS :, :] = blank

    def first(j, carry):
        r = pl.multiple_of(j * ROWS, ROWS)
        for p, (ref, at) in enumerate(refs):
            value = scale_ref[p, pl.ds(r, ROWS), :] * ref[at, pl.ds(r, ROWS), :]
            sq[p, pl.ds(r, ROWS), :] = value
            ea[p, pl.ds(r + ROWS, ROWS), :] = value
        return carry

    lax.fori_loop(0, rows // ROWS, first, 0)
    src, dst = ea, eb
    for sweep in range(1, SWEEPS):
        final = sweep == SWEEPS - 1

        def body(j, carry, src=src, dst=dst, final=final):
            r = pl.multiple_of(j * ROWS, ROWS)
            planes = [
                [src[p, pl.ds(r + ROWS, ROWS), lane(t)] for t in range(tiles)] for p in range(span)
            ]
            for p in range(span):
                for t in range(tiles):
                    beside = lateral(
                        planes,
                        p,
                        t,
                        src[p, pl.ds(r, ROWS), lane(t)],
                        src[p, pl.ds(r + 2 * ROWS, ROWS), lane(t)],
                    )
                    if p > 0:
                        beside = beside + planes[p - 1][t]
                    if p + 1 < span:
                        beside = beside + planes[p + 1][t]
                    here = pl.ds(r, ROWS)
                    value = (1.0 - OMEGA) * planes[p][t] + sq[p, here, lane(t)]
                    value = value + scale_ref[p, here, lane(t)] * beside
                    if not final:
                        dst[p, pl.ds(r + ROWS, ROWS), lane(t)] = value
                    elif p < span // 2:
                        lo_ref[p, here, lane(t)] = value
                    else:
                        hi_ref[p - span // 2, here, lane(t)] = value
            return carry

        lax.fori_loop(0, rows // ROWS, body, 0)
        src, dst = dst, src


def solve(order, extra, resid, scale):
    span, rows, depth = scale.shape
    half = jax.ShapeDtypeStruct((span // 2, rows, depth), jnp.float32)
    padded = pltpu.VMEM((span, rows + 2 * ROWS, depth), jnp.float32)
    return pl.pallas_call(
        functools.partial(solve_kernel, order),
        out_shape=(half, half),
        in_specs=[pl.BlockSpec(memory_space=pltpu.VMEM)] * 3,
        out_specs=(pl.BlockSpec(memory_space=pltpu.VMEM),) * 2,
        scratch_shapes=[pltpu.VMEM((span, rows, depth), jnp.float32), padded, padded],
        compiler_params=pltpu.CompilerParams(vmem_limit_bytes=24 << 20),
        cost_estimate=pl.CostEstimate(
            flops=SWEEPS * 40 * span * rows * depth,
            bytes_accessed=20 * span * rows * depth,
            transcendentals=0,
        ),
        name="solve",
    )(extra, resid, scale)


def image_kernel(order, part_0, part_1, part_2, diag_ref, resid_ref, image_ref, dots_ref):
    count, rows, depth = diag_ref.shape
    tiles = depth // LANES
    parts = (part_0, part_1, part_2)
    rim = RIM // ROWS
    start = lax.axis_index("colour") * rim
    steps = rows // ROWS

    def body(j, carry):
        upper, lower = carry
        r = pl.multiple_of(j * ROWS, ROWS)
        below = pl.multiple_of(jnp.maximum(j - 1, 0) * ROWS, ROWS)
        above = pl.multiple_of(jnp.minimum(j + 1, steps - 1) * ROWS, ROWS)
        has_below = (j > 0).astype(jnp.float32)
        has_above = (j + 1 < steps).astype(jnp.float32)
        own = ((j >= start) & (j < start + steps - rim)).astype(jnp.float32)
        here = pl.ds(r, ROWS)
        planes = [[parts[k][at, here, lane(t)] for t in range(tiles)] for k, at in order]
        for p in range(count):
            k, at = order[p + 1]
            for t in range(tiles):
                before = parts[k][at, pl.ds(below, ROWS), lane(t)] * has_below
                after = parts[k][at, pl.ds(above, ROWS), lane(t)] * has_above
                beside = lateral(planes, p + 1, t, before, after)
                beside = beside + planes[p][t] + planes[p + 2][t]
                centre = planes[p + 1][t]
                value = (6.0 + diag_ref[p, here, lane(t)]) * centre - beside
                image_ref[p, here, lane(t)] = value
                weighted = centre * own
                upper = upper + resid_ref[p, here, lane(t)] * weighted
                lower = lower + weighted * value
        return upper, lower

    zero = jnp.zeros((ROWS, LANES), jnp.float32)
    upper, lower = lax.fori_loop(0, steps, body, (zero, zero))
    at = lax.broadcasted_iota(jnp.int32, (ROWS, LANES), 0)
    dots_ref[...] = jnp.where(at == 0, jnp.sum(upper), jnp.sum(lower))


def image_of(order, parts, diag, resid):
    count, rows, depth = diag.shape
    return pl.pallas_call(
        functools.partial(image_kernel, order),
        out_shape=(
            jax.ShapeDtypeStruct((count, rows, depth), jnp.float32),
            jax.ShapeDtypeStruct((ROWS, LANES), jnp.float32),
        ),
        in_specs=[pl.BlockSpec(memory_space=pltpu.VMEM)] * 5,
        out_specs=(pl.BlockSpec(memory_space=pltpu.VMEM),) * 2,
        compiler_params=pltpu.CompilerParams(vmem_limit_bytes=16 << 20),
        cost_estimate=pl.CostEstimate(
            flops=80 * count * rows * depth,
            bytes_accessed=20 * count * rows * depth,
            transcendentals=0,
        ),
        name="image",
    )(*parts, diag, resid)


def alpha_of(dots_ref):
    return jnp.broadcast_to(dots_ref[0:1, :] / dots_ref[1:2, :], (ROWS, LANES))


def update_kernel(dots_ref, resid_ref, image_ref, first_ref, out_ref):
    count, rows, depth = resid_ref.shape
    alpha = alpha_of(dots_ref)

    def body(j, carry):
        here = pl.ds(pl.multiple_of(j * ROWS, ROWS), ROWS)
        for p in range(count):
            for t in range(depth // LANES):
                value = resid_ref[p, here, lane(t)] - alpha * image_ref[p, here, lane(t)]
                out_ref[p, here, lane(t)] = value
                if p == 0:
                    first_ref[0, here, lane(t)] = value
        return carry

    lax.fori_loop(0, rows // ROWS, body, 0)


def update(dots, resid, image):
    count, rows, depth = resid.shape
    return pl.pallas_call(
        update_kernel,
        out_shape=(
            jax.ShapeDtypeStruct((1, rows, depth), jnp.float32),
            jax.ShapeDtypeStruct(resid.shape, jnp.float32),
        ),
        in_specs=[pl.BlockSpec(memory_space=pltpu.VMEM)] * 3,
        out_specs=(pl.BlockSpec(memory_space=pltpu.VMEM),) * 2,
        compiler_params=pltpu.CompilerParams(vmem_limit_bytes=16 << 20),
        cost_estimate=pl.CostEstimate(
            flops=4 * count * rows * depth,
            bytes_accessed=12 * count * rows * depth,
            transcendentals=0,
        ),
        name="update",
    )(dots, resid, image)


def finish_kernel(
    order_0, order_1, dots_0, dots_1, a_0, a_1, a_2, b_0, b_1, b_2, resid_ref, image_ref,
    kept_ref, sent_ref, norm_ref,
):
    count, rows, depth = resid_ref.shape
    half = depth // 2
    me = lax.axis_index("colour")
    alpha_0 = alpha_of(dots_0)
    alpha_1 = alpha_of(dots_1)
    first, second = (a_0, a_1, a_2), (b_0, b_1, b_2)

    def body(j, acc):
        here = pl.ds(pl.multiple_of(me * RIM + j * ROWS, ROWS), ROWS)
        there = pl.ds(pl.multiple_of(j * ROWS, ROWS), ROWS)
        for out, side in ((kept_ref, me), (sent_ref, 1 - me)):
            for t in range(half // LANES):
                at_z = pl.ds(pl.multiple_of(side * half + t * LANES, LANES), LANES)
                for p in range(count):
                    k, at = order_0[p + 1]
                    m, to = order_1[p + 1]
                    u = alpha_0 * first[k][at, here, at_z] + alpha_1 * second[m][to, here, at_z]
                    q = resid_ref[p, here, at_z] - alpha_1 * image_ref[p, here, at_z]
                    out[0, p, there, lane(t)] = u
                    out[1, p, there, lane(t)] = q
                    acc = acc + q * q
        return acc

    steps = kept_ref.shape[2] // ROWS
    acc = lax.fori_loop(0, steps, body, jnp.zeros((ROWS, LANES), jnp.float32))
    norm_ref[...] = jnp.broadcast_to(jnp.sum(acc), (ROWS, LANES))


def finish(order_0, order_1, dots_0, dots_1, parts_0, parts_1, resid, image):
    count, rows, depth = resid.shape
    block = jax.ShapeDtypeStruct((2, count, rows - RIM, depth // 2), jnp.float32)
    return pl.pallas_call(
        functools.partial(finish_kernel, order_0, order_1),
        out_shape=(block, block, jax.ShapeDtypeStruct((ROWS, LANES), jnp.float32)),
        in_specs=[pl.BlockSpec(memory_space=pltpu.VMEM)] * 10,
        out_specs=(pl.BlockSpec(memory_space=pltpu.VMEM),) * 3,
        compiler_params=pltpu.CompilerParams(vmem_limit_bytes=24 << 20),
        cost_estimate=pl.CostEstimate(
            flops=8 * count * rows * depth,
            bytes_accessed=24 * count * rows * depth,
            transcendentals=0,
        ),
        name="finish",
    )(dots_0, dots_1, *parts_0, *parts_1, resid, image)


ORDER_0 = ((0, 0), (0, 1), (1, 0), (1, 1), (2, 0), (2, 1))
ORDER_1 = ((2, 0), (2, 1), (0, 0), (0, 1), (1, 0), (1, 1))


def shards(rhs, diagonal):
    colour = lax.axis_index("colour")
    device = lax.axis_index("sub")
    count = lax.axis_size("sub")
    nrhs, _, ny, _ = rhs.shape
    rows = ny // 2 + RIM
    begin = colour * (ny // 2 - RIM)
    to_right = [(i, i + 1) for i in range(count - 1)]
    to_left = [(i + 1, i) for i in range(count - 1)]

    source = lax.dynamic_slice_in_dim(rhs, begin, rows, 2)
    diag = lax.dynamic_slice_in_dim(diagonal, begin, rows, 1)
    diag_low = lax.ppermute(diag[-1:], "sub", to_right)
    low = [lax.ppermute(source[n, -1:], "sub", to_right) for n in range(nrhs)]
    diag_high = lax.ppermute(diag[:1], "sub", to_left)
    has_low = (device > 0).astype(jnp.float32)
    has_high = (device < count - 1).astype(jnp.float32)
    scale = OMEGA / (6.0 + diag)
    scale_0 = jnp.concatenate([has_low * (OMEGA / (6.0 + diag_low)), scale[:-1]], axis=0)
    scale_1 = jnp.concatenate([scale[1:], has_high * (OMEGA / (6.0 + diag_high))], axis=0)

    q = [source[n] for n in range(nrhs)]
    parts_0, parts_1, dots_0, dots_1 = [], [], [], []
    images, q1, high = [], [], []
    for n in range(nrhs):
        lo, hi = solve((-1, 0, 1, 2), low[n], q[n], scale_0)
        parts_0.append((lo, hi, lax.ppermute(lo, "sub", to_left)))
    for n in range(nrhs):
        image, dots = image_of(ORDER_0, parts_0[n], diag, q[n])
        images.append(image)
        dots_0.append(lax.psum(dots, ("colour", "sub")))
    for n in range(nrhs):
        edge, resid = update(dots_0[n], q[n], images[n])
        q1.append(resid)
        high.append(lax.ppermute(edge, "sub", to_left))
    for n in range(nrhs):
        lo, hi = solve((1, 2, 3, -1), high[n], q1[n], scale_1)
        parts_1.append((lo, hi, lax.ppermute(hi, "sub", to_right)))
    images = []
    for n in range(nrhs):
        image, dots = image_of(ORDER_1, parts_1[n], diag, q1[n])
        images.append(image)
        dots_1.append(lax.psum(dots, ("colour", "sub")))
    outs, norms = [], []
    for n in range(nrhs):
        kept, sent, norm = finish(
            ORDER_0, ORDER_1, dots_0[n], dots_1[n], parts_0[n], parts_1[n], q1[n], images[n]
        )
        got = lax.ppermute(sent, "colour", [(0, 1), (1, 0)])
        first = colour == 0
        below = jnp.where(first, kept, got)
        above = jnp.where(first, got, kept)
        outs.append(jnp.concatenate([below, above], axis=2))
        norms.append(norm[0, 0])
    solution = jnp.stack([out[0] for out in outs])
    residual = jnp.stack([out[1] for out in outs])
    squares = lax.psum(jnp.stack(norms), ("colour", "sub"))
    return solution, residual, jnp.sqrt(squares)


def solution(mesh):
    placed = (P(None, "sub", None, None), P("sub", None, None))
    return jax.shard_map(
        shards,
        mesh=mesh,
        in_specs=placed,
        out_specs=(P(None, "sub", None, "colour"), P(None, "sub", None, "colour"), P()),
        check_vma=False,
    )
```
